32 devices in a mesh: dp: 16 (over z, y, x), mp: 2 (over core).
Axes of the slice: x: 2, y: 2, z: 4, core: 2. Of those that a mesh axis runs over, the one named last changes fastest.
Arguments:
- points: bfloat16 [16384, 1024], P(('dp', 'mp')), may hold values from -6 to 6
- centroids: bfloat16 [4096, 1024], P('mp'), may hold values from -6 to 6
- assign: int32 [16384], P(('dp', 'mp')), may hold values from 0 to 4095
- keep_mask: int32 [16384], P(('dp', 'mp')), may hold values 0 or 1
Outputs:
- new_centroids: float32 [4096, 1024], P('mp')
- row_cost: float32 [16384], P(('dp', 'mp'))
The draws below stay inside these ranges and needn't reach their ends.
All inputs are finite; a program needn't handle non-finite values. No bound on the sum of `keep_mask` on one device may be relied on, other than what follows from the above.
Results may differ from the reference program's by a relative error of at most 0.0008.
Values may be sent and summed in bfloat16 or wider, within the bound.
A program may use at most 128 MiB of HBM per device.

```python
import math
import jax
import jax.numpy as jnp
import numpy as np
from jax import lax

D = 1024
K = 4096
ROWS = 16384


def place_ends(values, stream_key, smallest, high):
    longest = values.shape.index(max(values.shape))
    spots = []
    for shift in (0, 1):
        where = [jax.random.randint(jax.random.fold_in(stream_key, axis), (), 0, length) for axis, length in enumerate(values.shape)]
        where[longest] = (where[longest] + shift) % values.shape[longest]
        spots.append(tuple(where))
    return values.at[spots[0]].set(smallest).at[spots[1]].set(high)


def block_scale(own_key, dims, shards, smallest, high):
    level = 1.0
    for axis_at, shards_of in shards:
        draws = jax.random.uniform(jax.random.fold_in(jax.random.fold_in(own_key, 6), axis_at), (shards_of,), jnp.float32, smallest / len(shards), high / len(shards))
        level = level * jnp.repeat(jnp.exp(draws), dims[axis_at] // shards_of).reshape((-1,) + (1,) * (len(dims) - 1 - axis_at))
    return level


def cumulative_ranks(count, lean):
    portions = [(1 << 20) // math.isqrt(standing ** lean) + 1 for standing in range(1, count + 1)]
    width = 1 + sum(portions) // (1 << 30)
    return np.cumsum(np.array([max(1, weight // width) for weight in portions]))


def skewed_ids(own_key, extent, count, skew):
    grid = cumulative_ranks(count, skew)
    pick = jax.random.randint(jax.random.fold_in(own_key, 1), extent, 0, int(grid[count - 1]))
    standing = jnp.searchsorted(jnp.asarray(grid, jnp.int32), pick, side="right")
    return jax.random.permutation(jax.random.fold_in(own_key, 2), count)[standing].astype(jnp.int32)


def centred(own_key, shape, deviation, limit, cuts=(), kind=jnp.bfloat16):
    result = deviation * jax.random.normal(own_key, shape, jnp.float32)
    if cuts:
        result = result * block_scale(own_key, shape, cuts, -0.22, 0.18)
    return jnp.clip(result, -limit, limit).astype(kind)


def setup_inputs(seed: int = 0) -> dict:
    seeds = jax.random.split(jax.random.key(seed), 5)
    points = centred(seeds[0], (ROWS, D), 1.0, 6.0, ((0, 32),))
    centroids = centred(seeds[1], (K, D), 1.0, 6.0, ((0, 2),))
    assign = place_ends(skewed_ids(seeds[2], (ROWS,), K, 2), jax.random.fold_in(seeds[2], 3), 0, K - 1).astype(jnp.int32)
    keep_mask = place_ends((jax.random.randint(seeds[3], (ROWS,), 0, 4) < 3).astype(jnp.int32), jax.random.fold_in(seeds[3], 1), 0, 1)
    return dict(points=points, centroids=centroids, assign=assign, keep_mask=keep_mask)


def reference(points, centroids, assign, keep_mask):
    cent_f = centroids.astype(jnp.float32)
    cent_sq = jnp.sum(cent_f * cent_f, axis=1)
    block = math.gcd(ROWS, 1024)
    blocks = points.reshape(ROWS // block, block, D)

    def cost_block(group_rows):
        point_f = group_rows.astype(jnp.float32)
        point_sq = jnp.sum(point_f * point_f, axis=1)
        inner = jnp.dot(group_rows, centroids.T, preferred_element_type=jnp.float32)
        dist = point_sq[:, None] - 2.0 * inner + cent_sq[None, :]
        return jnp.min(dist, axis=1) / D

    row_cost = lax.map(cost_block, blocks).reshape(ROWS)
    weights = keep_mask.astype(jnp.float32)
    sums = jax.ops.segment_sum(points.astype(jnp.float32) * weights[:, None], assign, num_segments=K)
    counts = jax.ops.segment_sum(weights, assign, num_segments=K)
    fresh = sums / jnp.maximum(counts, 1.0)[:, None]
    new_centroids = jnp.where(counts[:, None] > 0.5, fresh, cent_f)
    return new_centroids, row_cost
```

```python
import functools

import jax
import jax.numpy as jnp
from jax import lax
from jax.experimental import pallas as pl
from jax.experimental.pallas import tpu as pltpu
from jax.sharding import Mesh
from jax.sharding import PartitionSpec as P

STEPS = 32000.0
TINY = 2.0**-100
EXTRA = 8
PLANE = 4
LANES = 128


def remote(src, dst, send, recv, device):
    return pltpu.make_async_remote_copy(
        src_ref=src,
        dst_ref=dst,
        send_sem=send,
        recv_sem=recv,
        device_id=device,
        device_id_type=pl.DeviceIdType.MESH,
    )


def greet(peers):
    barrier = pltpu.get_barrier_semaphore()
    for peer in peers:
        pl.semaphore_signal(barrier, inc=1, device_id=peer, device_id_type=pl.DeviceIdType.MESH)
    pl.semaphore_wait(barrier, len(peers))


def update_kernel(
    z_n, shard_rows, p_ref, id_ref, prior_ref, out_ref,
    near, idn, acc, mrecv, red, zrecv,
    ps, pr, ids_s, ids_r, ms, mr, zs, zr, gs, gr, xs, xr, ys, yr, ds_, dr,
):
    z, q, m = lax.axis_index("z"), lax.axis_index("q"), lax.axis_index("mp")
    nx = q + 1 - 2 * lax.rem(q, 2)
    ny = lax.rem(q + 2, PLANE)
    nd = ny + 1 - 2 * lax.rem(ny, 2)
    other = 1 - m
    rows, width = p_ref.shape
    block = prior_ref.shape[0]
    half = rows // 2
    peers = [(z, nx, m), (z, ny, m), (z, nd, m), (z, q, other)]
    greet(peers + [(lax.rem(z + d, z_n), q, m) for d in range(1, z_n)])

    id_copies = [
        remote(id_ref, idn.at[k], ids_s.at[k], ids_r.at[k], (z, to, m))
        for k, to in enumerate((nx, ny, nd))
    ]
    for c in id_copies:
        c.start()
    lo, hi = pl.ds(0, half), pl.ds(half, half)

    def piece(k, src, slot, part, to):
        return remote(src, near.at[slot, part], ps.at[k], pr.at[k], (z, to, m))

    a = piece(0, p_ref.at[lo], 0, lo, nx)
    c = piece(1, p_ref.at[hi], 1, hi, ny)
    b = piece(2, p_ref.at[hi], 0, hi, nx)
    d_ = piece(3, p_ref.at[lo], 1, lo, ny)
    e = piece(4, near.at[0, lo], 2, lo, ny)
    f = piece(5, near.at[1, hi], 2, hi, nx)
    for copy in (a, c, b, d_):
        copy.start()

    def add(ids, pts, first):
        def tile(t, carry):
            base = (t // z_n) * shard_rows + (lax.rem(t, z_n) * PLANE + q) * block
            row = base + lax.broadcasted_iota(jnp.int32, (block, rows), 0)
            hit = jnp.where(row == ids[0:1, :], 1.0, 0.0)
            part = jnp.dot(hit.astype(jnp.bfloat16), pts[...], preferred_element_type=jnp.float32)
            count = jnp.broadcast_to(jnp.sum(hit, axis=1, keepdims=True), (block, LANES))
            if first:
                acc[t, :, :width] = part
                acc[t, :, width:] = count
            else:
                acc[t, :, :width] += part
                acc[t, :, width:] += count
            return carry

        lax.fori_loop(0, 2 * z_n, tile, 0)

    add(id_ref, p_ref, True)
    a.wait_recv()
    e.start()
    c.wait_recv()
    f.start()
    for copy in id_copies:
        copy.wait_recv()
    b.wait_recv()
    add(idn.at[0], near.at[0], False)
    d_.wait_recv()
    add(idn.at[1], near.at[1], False)
    e.wait_recv()
    f.wait_recv()
    add(idn.at[2], near.at[2], False)

    mcopy = remote(acc.at[pl.ds(other * z_n, z_n)], mrecv, ms, mr, (z, q, other))
    mcopy.start()
    mcopy.wait_recv()

    zcopies = []
    for k in range(1, z_n + 1):
        to = lax.rem(z + k, z_n)
        red[to] = acc[m * z_n + to] + mrecv[to]
        if k < z_n:
            copy = remote(red.at[to], zrecv.at[k - 1], zs.at[k - 1], zr.at[k - 1], (to, q, m))
            copy.start()
            zcopies.append(copy)
    for k in range(1, z_n):
        zcopies[k - 1].wait_recv()
        red[z] += zrecv[k - 1]

    sums = red[z, :, :width]
    count = red[z, :, width : width + 1]
    fresh = jnp.where(
        count > 0.5, sums / jnp.maximum(count, 1.0), prior_ref[...].astype(jnp.float32)
    )
    own = z * PLANE + q
    half_w = width // 2
    top = jnp.max(jnp.abs(fresh), axis=1, keepdims=True)
    power = jnp.ceil(jnp.log2(jnp.maximum(top, TINY)))
    code = jnp.floor(fresh * jnp.exp2(-power) * STEPS + 0.5).astype(jnp.int32)
    out_ref[own, :block] = (code[:, :half_w] << 16) | (code[:, half_w:] & 0xFFFF)
    at_row = lax.broadcasted_iota(jnp.int32, (block, LANES), 0)
    at_lane = lax.broadcasted_iota(jnp.int32, (block, LANES), 1)
    flat = jnp.sum(jnp.where(at_row == at_lane, power, 0.0), axis=0, keepdims=True)
    out_ref[own, block:] = jnp.zeros((EXTRA, half_w), jnp.int32)
    out_ref[own, block:, :LANES] = jnp.broadcast_to(flat.astype(jnp.int32), (EXTRA, LANES))

    def pass_on(index, send, recv, device):
        copy = remote(out_ref.at[index], out_ref.at[index], send, recv, device)
        copy.start()
        return copy

    gcopies = [
        pass_on(own, gs.at[k - 1], gr.at[k - 1], (lax.rem(z + k, z_n), q, m))
        for k in range(1, z_n)
    ]
    xc, yc, dc = [], [], []

    def relay(k):
        base = lax.rem(z + z_n - k, z_n) * PLANE
        if k % 2 == 0:
            xc[k].wait_recv()
            dc.append(pass_on(base + nx, ds_.at[k], dr.at[k], (z, ny, m)))
        else:
            yc[k].wait_recv()
            dc.append(pass_on(base + ny, ds_.at[k], dr.at[k], (z, nx, m)))

    for k in range(z_n):
        mine = lax.rem(z + z_n - k, z_n) * PLANE + q
        if k > 0:
            gcopies[k - 1].wait_recv()
        xc.append(pass_on(mine, xs.at[k], xr.at[k], (z, nx, m)))
        yc.append(pass_on(mine, ys.at[k], yr.at[k], (z, ny, m)))
        if k > 0:
            relay(k - 1)
    relay(z_n - 1)
    for k in range(z_n):
        if k % 2 == 0:
            yc[k].wait_recv()
        else:
            xc[k].wait_recv()
        dc[k].wait_recv()
    for copy in id_copies + [a, b, c, d_, e, f, mcopy] + zcopies + gcopies + xc + yc + dc:
        copy.wait_send()


def shards(points, centroids, assign, keep_mask):
    rows, width = points.shape
    shard_rows = centroids.shape[0]
    z_n = lax.axis_size("z")
    dp_n = z_n * PLANE
    block = shard_rows // dp_n
    own = lax.axis_index("z") * PLANE + lax.axis_index("q")
    ids = jnp.where(keep_mask > 0, assign, -1)
    ids = jnp.broadcast_to(ids[None, :], (8, rows))
    prior = lax.dynamic_slice_in_dim(centroids, own * block, block, 0)
    vmem = pl.BlockSpec(memory_space=pltpu.VMEM)
    dma = pltpu.SemaphoreType.DMA
    wide = width + LANES
    back = pl.pallas_call(
        functools.partial(update_kernel, z_n, shard_rows),
        out_shape=jax.ShapeDtypeStruct((dp_n, block + EXTRA, width // 2), jnp.int32),
        in_specs=[vmem] * 3,
        out_specs=vmem,
        scratch_shapes=[
            pltpu.VMEM((3, rows, width), points.dtype),
            pltpu.VMEM((3, 8, rows), jnp.int32),
            pltpu.VMEM((2 * z_n, block, wide), jnp.float32),
            pltpu.VMEM((z_n, block, wide), jnp.float32),
            pltpu.VMEM((z_n, block, wide), jnp.float32),
            pltpu.VMEM((z_n - 1, block, wide), jnp.float32),
            dma((6,)), dma((6,)), dma((3,)), dma((3,)), dma, dma,
            dma((z_n - 1,)), dma((z_n - 1,)), dma((z_n - 1,)), dma((z_n - 1,)),
            dma((z_n,)), dma((z_n,)), dma((z_n,)), dma((z_n,)), dma((z_n,)), dma((z_n,)),
        ],
        compiler_params=pltpu.CompilerParams(
            collective_id=0, has_side_effects=True, vmem_limit_bytes=48 * 1024 * 1024
        ),
        cost_estimate=pl.CostEstimate(
            flops=0, bytes_accessed=200 * 1024 * 1024, transcendentals=0
        ),
    )(points, ids, prior)
    codes = back[:, :block]
    powers = back[:, block, :block].astype(jnp.float32)
    scale = (jnp.exp2(powers) / STEPS)[:, :, None]
    pair = jnp.concatenate([codes >> 16, (codes << 16) >> 16], axis=2)
    new_centroids = (pair.astype(jnp.float32) * scale).reshape(shard_rows, width)

    piece = lax.all_gather(centroids, "mp", axis=0, tiled=True)
    inner = lax.dot_general(
        points, piece, (((1,), (1,)), ((), ())), preferred_element_type=jnp.float32
    )
    point_f = points.astype(jnp.float32)
    point_sq = jnp.sum(point_f * point_f, axis=1)
    piece_f = piece.astype(jnp.float32)
    cent_sq = jnp.sum(piece_f * piece_f, axis=1)
    dist = point_sq[:, None] - 2.0 * inner + cent_sq[None, :]
    row_cost = jnp.min(dist, axis=1) / width
    return new_centroids, row_cost


def solution(mesh):
    dp, mp = mesh.shape["dp"], mesh.shape["mp"]
    grid = Mesh(mesh.devices.reshape(dp // PLANE, PLANE, mp), ("z", "q", "mp"))
    rows = ("z", "q", "mp")
    in_specs = (P(rows, None), P("mp", None), P(rows), P(rows))
    out_specs = (P("mp", None), P(rows))
    return jax.shard_map(shards, mesh=grid, in_specs=in_specs, out_specs=out_specs, check_vma=False)
```

```python
import functools

import jax
import jax.numpy as jnp
from jax import lax
from jax.experimental import pallas as pl
from jax.experimental.pallas import tpu as pltpu
from jax.sharding import Mesh
from jax.sharding import PartitionSpec as P

STEPS = 32000.0
TINY = 2.0**-100
EXTRA = 8
PLANE = 4
LANES = 128
CHUNKS = 2
MESH = pl.DeviceIdType.MESH


def remote(src, dst, send, recv, device):
    return pltpu.make_async_remote_copy(
        src_ref=src, dst_ref=dst, send_sem=send, recv_sem=recv, device_id=device, device_id_type=MESH
    )


def update_kernel(
    z_n, shard_rows, p_ref, id_ref, prior_ref, c_ref, out_ref, low_ref,
    crecv, near, idn, acc, mrecv, red, zright, zleft,
    cs, cr, ids_s, ids_r, ps, pr, ms, mr, rs, rr, ls, lr,
    grs, grr, gls, glr, xs, xr, ys, yr, ds_, dr,
):
    z, q, m = lax.axis_index("z"), lax.axis_index("q"), lax.axis_index("mp")
    nx = q + 1 - 2 * lax.rem(q, 2)
    ny = lax.rem(q + 2, PLANE)
    nd = ny + 1 - 2 * lax.rem(ny, 2)
    other = 1 - m
    rows, width = p_ref.shape
    block = prior_ref.shape[0]
    half = rows // 2
    part = width // CHUNKS
    code_w = part // 2
    last = z_n - 1
    up, down = lax.rem(z + 1, z_n), lax.rem(z + last, z_n)

    barrier = pltpu.get_barrier_semaphore()
    peers = [(z, nx, m), (z, ny, m), (z, nd, m), (z, q, other), (up, q, m), (down, q, m)]
    for peer in peers:
        pl.semaphore_signal(barrier, inc=1, device_id=peer, device_id_type=MESH)
    pl.semaphore_wait(barrier, len(peers))

    id_copies = [
        remote(id_ref, idn.at[k], ids_s.at[k], ids_r.at[k], (z, to, m))
        for k, to in enumerate((nx, ny, nd))
    ]
    lo, hi = pl.ds(0, half), pl.ds(half, half)

    def gather_copies(c):
        cols = pl.ds(c * part, part)

        def piece(k, src, slot, span, to):
            return remote(src, near.at[c, slot, span], ps.at[c, k], pr.at[c, k], (z, to, m))

        return (
            piece(0, p_ref.at[lo, cols], 0, lo, nx),
            piece(1, p_ref.at[hi, cols], 1, hi, ny),
            piece(2, p_ref.at[hi, cols], 0, hi, nx),
            piece(3, p_ref.at[lo, cols], 1, lo, ny),
            piece(4, near.at[c, 0, lo], 2, lo, ny),
            piece(5, near.at[c, 1, hi], 2, hi, nx),
        )

    gathers = [gather_copies(c) for c in range(CHUNKS)]

    def width_of(c):
        return part + (LANES if c == 0 else 0)

    def add(c, ids, pts, first):
        def tile(t, carry):
            base = (t // z_n) * shard_rows + (lax.rem(t, z_n) * PLANE + q) * block
            row = base + lax.broadcasted_iota(jnp.int32, (block, rows), 0)
            hit = jnp.where(row == ids[0:1, :], 1.0, 0.0)
            s = jnp.dot(hit.astype(jnp.bfloat16), pts[...], preferred_element_type=jnp.float32)
            if first:
                acc[c, t, :, :part] = s
            else:
                acc[c, t, :, :part] += s
            if c == 0:
                count = jnp.broadcast_to(jnp.sum(hit, axis=1, keepdims=True), (block, LANES))
                if first:
                    acc[c, t, :, part:] = count
                else:
                    acc[c, t, :, part:] += count
            return carry

        lax.fori_loop(0, 2 * z_n, tile, 0)

    ctile = 256

    def lowest(cents, first):
        def tile(t, best):
            tile_ref = cents[pl.ds(pl.multiple_of(t * ctile, ctile), ctile), :]
            wide = tile_ref.astype(jnp.float32)
            sq = jnp.sum(wide * wide, axis=1, keepdims=True)
            inner = lax.dot_general(
                tile_ref, p_ref[...], (((1,), (1,)), ((), ())), preferred_element_type=jnp.float32
            )
            return jnp.minimum(best, jnp.min(sq - 2.0 * inner, axis=0, keepdims=True))

        start = jnp.full((1, rows), jnp.inf, jnp.float32) if first else low_ref[0:1, :]
        best = lax.fori_loop(0, shard_rows // ctile, tile, start)
        low_ref[...] = jnp.broadcast_to(best, low_ref.shape)

    ccopy = remote(c_ref, crecv, cs, cr, (z, q, other))
    for copy in id_copies + list(gathers[0][:4]):
        copy.start()
    ccopy.start()

    mcopies = []
    for c in range(CHUNKS):
        a, b2, b, d, e, f = gathers[c]
        add(c, id_ref, p_ref.at[:, pl.ds(c * part, part)], True)
        a.wait_recv()
        e.start()
        b2.wait_recv()
        f.start()
        if c + 1 < CHUNKS:
            for copy in gathers[c + 1][:4]:
                copy.start()
        if c == 0:
            lowest(c_ref, True)
            for copy in id_copies:
                copy.wait_recv()
        b.wait_recv()
        add(c, idn.at[0], near.at[c, 0], False)
        d.wait_recv()
        add(c, idn.at[1], near.at[c, 1], False)
        if c == CHUNKS - 1:
            ccopy.wait_recv()
            lowest(crecv, False)
        e.wait_recv()
        f.wait_recv()
        add(c, idn.at[2], near.at[c, 2], False)
        w = pl.ds(0, width_of(c))
        copy = remote(
            acc.at[c, pl.ds(other * z_n, z_n), :, w], mrecv.at[c, :, :, w],
            ms.at[c], mr.at[c], (z, q, other),
        )
        copy.start()
        mcopies.append(copy)

    def right(c, t):
        w = pl.ds(0, width_of(c))
        return remote(
            red.at[c, t, :, w], zright.at[c, t, :, w], rs.at[c, t], rr.at[c, t], (up, q, m)
        )

    def left(c, t):
        w = pl.ds(0, width_of(c))
        return remote(
            red.at[c, t, :, w], zleft.at[c, t, :, w], ls.at[c, t], lr.at[c, t], (down, q, m)
        )

    for c in range(CHUNKS):
        mcopies[c].wait_recv()
        w = width_of(c)
        for t in range(z_n):
            red[c, t, :, :w] = acc[c, m * z_n + t, :, :w] + mrecv[c, t, :, :w]

    for s in range(last):
        for c in range(CHUNKS):
            w = width_of(c)
            for far, go, land, send, more in (
                (last - s, z < last - s, zright, right, z > 0),
                (s, z > s, zleft, left, z < last),
            ):

                @pl.when(go)
                def _(c=c, w=w, far=far, land=land, send=send, more=more):
                    @pl.when(more)
                    def _():
                        send(c, far).wait_recv()
                        red[c, far, :, :w] += land[c, far, :, :w]

                    send(c, far).start()

    own = z * PLANE + q

    def xcopy(c, n, to_q):
        at = out_ref.at[c, n * PLANE + to_q]
        return remote(at, at, xs.at[c, n], xr.at[c, n], (z, nx, m))

    def ycopy(c, n, to_q):
        at = out_ref.at[c, n * PLANE + to_q]
        return remote(at, at, ys.at[c, n], yr.at[c, n], (z, ny, m))

    def dcopy(c, n, by_x):
        at = out_ref.at[c, n * PLANE + (nx if by_x else ny)]
        return remote(at, at, ds_.at[c, n], dr.at[c, n], (z, ny if by_x else nx, m))

    def gright(c, n):
        at = out_ref.at[c, n * PLANE + q]
        return remote(at, at, grs.at[c, n], grr.at[c, n], (up, q, m))

    def gleft(c, n):
        at = out_ref.at[c, n * PLANE + q]
        return remote(at, at, gls.at[c, n], glr.at[c, n], (down, q, m))

    count = None
    for c in range(CHUNKS):
        w = width_of(c)

        @pl.when(z > 0)
        def _(c=c, w=w):
            right(c, z).wait_recv()
            red[c, z, :, :w] += zright[c, z, :, :w]

        @pl.when(z < last)
        def _(c=c, w=w):
            left(c, z).wait_recv()
            red[c, z, :, :w] += zleft[c, z, :, :w]

        if c == 0:
            count = red[c, z, :, part : part + 1]
        prior = prior_ref[:, c * part : (c + 1) * part].astype(jnp.float32)
        fresh = jnp.where(count > 0.5, red[c, z, :, :part] / jnp.maximum(count, 1.0), prior)
        top = jnp.max(jnp.abs(fresh), axis=1, keepdims=True)
        power = jnp.ceil(jnp.log2(jnp.maximum(top, TINY)))
        code = jnp.floor(fresh * jnp.exp2(-power) * STEPS + 0.5).astype(jnp.int32)
        out_ref[c, own, :block] = (code[:, :code_w] << 16) | (code[:, code_w:] & 0xFFFF)
        at_row = lax.broadcasted_iota(jnp.int32, (block, LANES), 0)
        at_lane = lax.broadcasted_iota(jnp.int32, (block, LANES), 1)
        flat = jnp.sum(jnp.where(at_row == at_lane, power, 0.0), axis=0, keepdims=True)
        out_ref[c, own, block:] = jnp.zeros((EXTRA, code_w), jnp.int32)
        out_ref[c, own, block:, :LANES] = jnp.broadcast_to(flat.astype(jnp.int32), (EXTRA, LANES))

        @pl.when(z < last)
        def _(c=c):
            gright(c, z).start()

        @pl.when(z > 0)
        def _(c=c):
            gleft(c, z).start()

        xcopy(c, z, q).start()
        ycopy(c, z, q).start()

    def relay(c, n, by_x):
        if by_x:
            xcopy(c, n, nx).wait_recv()
        else:
            ycopy(c, n, ny).wait_recv()
        dcopy(c, n, by_x).start()

    def settle(c, n, by_x):
        if by_x:
            ycopy(c, n, ny).wait_recv()
        else:
            xcopy(c, n, nx).wait_recv()
        dcopy(c, n, by_x).wait_recv()

    def each(k, c, action):
        if k == 0:
            action(c, z, c % 2 == 0)
            return

        @pl.when(z >= k)
        def _():
            action(c, z - k, k % 2 == 0)

        @pl.when(z + k <= last)
        def _():
            action(c, z + k, k % 2 == 1)

    for k in range(z_n):
        for c in range(CHUNKS):
            if k > 0:

                @pl.when(z >= k)
                def _(c=c, k=k):
                    gright(c, z - k).wait_recv()

                    @pl.when(z < last)
                    def _():
                        gright(c, z - k).start()

                    xcopy(c, z - k, q).start()
                    ycopy(c, z - k, q).start()

                @pl.when(z + k <= last)
                def _(c=c, k=k):
                    gleft(c, z + k).wait_recv()

                    @pl.when(z > 0)
                    def _():
                        gleft(c, z + k).start()

                    xcopy(c, z + k, q).start()
                    ycopy(c, z + k, q).start()

        if k > 0:
            for c in range(CHUNKS):
                each(k - 1, c, relay)
    for c in range(CHUNKS):
        each(last, c, relay)
    for k in range(z_n):
        for c in range(CHUNKS):
            each(k, c, settle)

    for copy in id_copies + [ccopy] + mcopies:
        copy.wait_send()
    for c in range(CHUNKS):
        for copy in gathers[c]:
            copy.wait_send()
        for t in range(z_n):

            @pl.when(z < t)
            def _(c=c, t=t):
                right(c, t).wait_send()

            @pl.when(z > t)
            def _(c=c, t=t):
                left(c, t).wait_send()

            @pl.when((z >= t) & (z < last))
            def _(c=c, t=t):
                gright(c, t).wait_send()

            @pl.when((z <= t) & (z > 0))
            def _(c=c, t=t):
                gleft(c, t).wait_send()

            xcopy(c, t, q).wait_send()
            ycopy(c, t, q).wait_send()
            dcopy(c, t, True).wait_send()


def shards(points, centroids, assign, keep_mask):
    rows, width = points.shape
    shard_rows = centroids.shape[0]
    z_n = lax.axis_size("z")
    dp_n = z_n * PLANE
    block = shard_rows // dp_n
    own = lax.axis_index("z") * PLANE + lax.axis_index("q")
    ids = jnp.where(keep_mask > 0, assign, -1)
    ids = jnp.broadcast_to(ids[None, :], (8, rows))
    prior = lax.dynamic_slice_in_dim(centroids, own * block, block, 0)
    vmem = pl.BlockSpec(memory_space=pltpu.VMEM)
    dma = pltpu.SemaphoreType.DMA
    part = width // CHUNKS
    wide = part + LANES
    per = dma((CHUNKS, z_n))
    back, low = pl.pallas_call(
        functools.partial(update_kernel, z_n, shard_rows),
        out_shape=(
            jax.ShapeDtypeStruct((CHUNKS, dp_n, block + EXTRA, part // 2), jnp.int32),
            jax.ShapeDtypeStruct((8, rows), jnp.float32),
        ),
        in_specs=[vmem] * 4,
        out_specs=(vmem, vmem),
        scratch_shapes=[
            pltpu.VMEM((shard_rows, width), centroids.dtype),
            pltpu.VMEM((CHUNKS, 3, rows, part), points.dtype),
            pltpu.VMEM((3, 8, rows), jnp.int32),
            pltpu.VMEM((CHUNKS, 2 * z_n, block, wide), jnp.float32),
            pltpu.VMEM((CHUNKS, z_n, block, wide), jnp.float32),
            pltpu.VMEM((CHUNKS, z_n, block, wide), jnp.float32),
            pltpu.VMEM((CHUNKS, z_n, block, wide), jnp.float32),
            pltpu.VMEM((CHUNKS, z_n, block, wide), jnp.float32),
            dma, dma, dma((3,)), dma((3,)), dma((CHUNKS, 6)), dma((CHUNKS, 6)),
            dma((CHUNKS,)), dma((CHUNKS,)),
            per, per, per, per, per, per, per, per, per, per, per, per, per, per,
        ],
        compiler_params=pltpu.CompilerParams(
            collective_id=0, has_side_effects=True, vmem_limit_bytes=56 * 1024 * 1024
        ),
        cost_estimate=pl.CostEstimate(
            flops=0, bytes_accessed=200 * 1024 * 1024, transcendentals=0
        ),
    )(points, ids, prior, centroids)
    codes = back[:, :, :block]
    powers = back[:, :, block, :block].astype(jnp.float32)
    scale = (jnp.exp2(powers) / STEPS)[:, :, :, None]
    pieces = []
    for c in range(CHUNKS):
        pieces += [(codes[c] >> 16) * scale[c], ((codes[c] << 16) >> 16) * scale[c]]
    new_centroids = jnp.concatenate(pieces, axis=2).reshape(shard_rows, width)
    point_f = points.astype(jnp.float32)
    point_sq = jnp.sum(point_f * point_f, axis=1)
    return new_centroids, (point_sq + low[0]) / width


def solution(mesh):
    dp, mp = mesh.shape["dp"], mesh.shape["mp"]
    grid = Mesh(mesh.devices.reshape(dp // PLANE, PLANE, mp), ("z", "q", "mp"))
    rows = ("z", "q", "mp")
    in_specs = (P(rows, None), P("mp", None), P(rows), P(rows))
    out_specs = (P("mp", None), P(rows))
    return jax.shard_map(shards, mesh=grid, in_specs=in_specs, out_specs=out_specs, check_vma=False)
```

```python
import functools

import jax
import jax.numpy as jnp
from jax import lax
from jax.experimental import pallas as pl
from jax.experimental.pallas import tpu as pltpu
from jax.sharding import Mesh
from jax.sharding import PartitionSpec as P

STEPS = 32000.0
TINY = 2.0**-100
EXTRA = 8
PLANE = 4
LANES = 128
CHUNKS = 2
MESH = pl.DeviceIdType.MESH


def remote(src, dst, send, recv, device):
    return pltpu.make_async_remote_copy(
        src_ref=src, dst_ref=dst, send_sem=send, recv_sem=recv, device_id=device, device_id_type=MESH
    )


def update_kernel(
    z_n, shard_rows, p_ref, id_ref, prior_ref, c_ref, out_ref, low_ref,
    crecv, near, idn, acc, mrecv, red, zright,
    cs, cr, ids_s, ids_r, ps, pr, ms, mr, rs, rr,
    grs, grr, gls, glr, xs, xr, ys, yr, ds_, dr,
):
    z, q, m = lax.axis_index("z"), lax.axis_index("q"), lax.axis_index("mp")
    nx = q + 1 - 2 * lax.rem(q, 2)
    ny = lax.rem(q + 2, PLANE)
    nd = ny + 1 - 2 * lax.rem(ny, 2)
    other = 1 - m
    rows, width = p_ref.shape
    block = prior_ref.shape[0]
    half = rows // 2
    part = width // CHUNKS
    code_w = part // 2
    last = z_n - 1
    up, down = lax.rem(z + 1, z_n), lax.rem(z + last, z_n)

    barrier = pltpu.get_barrier_semaphore()
    peers = [(z, nx, m), (z, ny, m), (z, nd, m), (z, q, other)]
    peers += [(lax.rem(z + k, z_n), q, m) for k in range(1, z_n)]
    for peer in peers:
        pl.semaphore_signal(barrier, inc=1, device_id=peer, device_id_type=MESH)
    pl.semaphore_wait(barrier, len(peers))

    id_copies = [
        remote(id_ref, idn.at[k], ids_s.at[k], ids_r.at[k], (z, to, m))
        for k, to in enumerate((nx, ny, nd))
    ]
    lo, hi = pl.ds(0, half), pl.ds(half, half)

    def gather_copies(c):
        cols = pl.ds(c * part, part)

        def piece(k, src, slot, span, to):
            return remote(src, near.at[c, slot, span], ps.at[c, k], pr.at[c, k], (z, to, m))

        return (
            piece(0, p_ref.at[lo, cols], 0, lo, nx),
            piece(1, p_ref.at[hi, cols], 1, hi, ny),
            piece(2, p_ref.at[hi, cols], 0, hi, nx),
            piece(3, p_ref.at[lo, cols], 1, lo, ny),
            piece(4, near.at[c, 0, lo], 2, lo, ny),
            piece(5, near.at[c, 1, hi], 2, hi, nx),
        )

    gathers = [gather_copies(c) for c in range(CHUNKS)]

    def width_of(c):
        return part + (LANES if c == 0 else 0)

    def add(c, ids, pts, first):
        def tile(t, carry):
            base = (t // z_n) * shard_rows + (lax.rem(t, z_n) * PLANE + q) * block
            row = base + lax.broadcasted_iota(jnp.int32, (block, rows), 0)
            hit = jnp.where(row == ids[0:1, :], 1.0, 0.0)
            s = jnp.dot(hit.astype(jnp.bfloat16), pts[...], preferred_element_type=jnp.float32)
            if first:
                acc[c, t, :, :part] = s
            else:
                acc[c, t, :, :part] += s
            if c == 0:
                count = jnp.broadcast_to(jnp.sum(hit, axis=1, keepdims=True), (block, LANES))
                if first:
                    acc[c, t, :, part:] = count
                else:
                    acc[c, t, :, part:] += count
            return carry

        lax.fori_loop(0, 2 * z_n, tile, 0)

    ctile = 256

    def lowest(cents, first):
        def tile(t, best):
            tile_ref = cents[pl.ds(pl.multiple_of(t * ctile, ctile), ctile), :]
            wide = tile_ref.astype(jnp.float32)
            sq = jnp.sum(wide * wide, axis=1, keepdims=True)
            inner = lax.dot_general(
                tile_ref, p_ref[...], (((1,), (1,)), ((), ())), preferred_element_type=jnp.float32
            )
            return jnp.minimum(best, jnp.min(sq - 2.0 * inner, axis=0, keepdims=True))

        start = jnp.full((1, rows), jnp.inf, jnp.float32) if first else low_ref[0:1, :]
        best = lax.fori_loop(0, shard_rows // ctile, tile, start)
        low_ref[...] = jnp.broadcast_to(best, low_ref.shape)

    ccopy = remote(c_ref, crecv, cs, cr, (z, q, other))
    for copy in id_copies + list(gathers[0][:4]):
        copy.start()
    ccopy.start()

    mcopies = []

    def open_gather(c):
        a, b2, _, _, e, f = gathers[c]
        add(c, id_ref, p_ref.at[:, pl.ds(c * part, part)], True)
        a.wait_recv()
        e.start()
        b2.wait_recv()
        f.start()
        if c + 1 < CHUNKS:
            for copy in gathers[c + 1][:4]:
                copy.start()

    def close_gather(c):
        _, _, b, d, e, f = gathers[c]
        if c == 0:
            lowest(c_ref, True)
            for copy in id_copies:
                copy.wait_recv()
        b.wait_recv()
        add(c, idn.at[0], near.at[c, 0], False)
        d.wait_recv()
        add(c, idn.at[1], near.at[c, 1], False)
        if c == 0:
            ccopy.wait_recv()
            lowest(crecv, False)
        e.wait_recv()
        f.wait_recv()
        add(c, idn.at[2], near.at[c, 2], False)
        w = pl.ds(0, width_of(c))
        copy = remote(
            acc.at[c, pl.ds(other * z_n, z_n), :, w], mrecv.at[c, :, :, w],
            ms.at[c], mr.at[c], (z, q, other),
        )
        copy.start()
        mcopies.append(copy)

    def direct(c, k):
        w = pl.ds(0, width_of(c))
        to = lax.rem(z + k, z_n)
        return remote(
            red.at[c, to, :, w], zright.at[c, k, :, w], rs.at[c, k], rr.at[c, k], (to, q, m)
        )

    def combine(c):
        mcopies[c].wait_recv()
        w = width_of(c)
        for k in range(1, z_n + 1):
            t = lax.rem(z + k, z_n)
            red[c, t, :, :w] = acc[c, m * z_n + t, :, :w] + mrecv[c, t, :, :w]
            if k < z_n:
                direct(c, k).start()

    own = z * PLANE + q

    def xcopy(c, n, to_q):
        at = out_ref.at[c, n * PLANE + to_q]
        return remote(at, at, xs.at[c, n], xr.at[c, n], (z, nx, m))

    def ycopy(c, n, to_q):
        at = out_ref.at[c, n * PLANE + to_q]
        return remote(at, at, ys.at[c, n], yr.at[c, n], (z, ny, m))

    def dcopy(c, n, by_x):
        at = out_ref.at[c, n * PLANE + (nx if by_x else ny)]
        return remote(at, at, ds_.at[c, n], dr.at[c, n], (z, ny if by_x else nx, m))

    def gright(c, n):
        at = out_ref.at[c, n * PLANE + q]
        return remote(at, at, grs.at[c, n], grr.at[c, n], (up, q, m))

    def gleft(c, n):
        at = out_ref.at[c, n * PLANE + q]
        return remote(at, at, gls.at[c, n], glr.at[c, n], (down, q, m))

    def publish(c, count):
        w = width_of(c)

        for k in range(1, z_n):
            direct(c, k).wait_recv()
            red[c, z, :, :w] += zright[c, k, :, :w]

        if c == 0:
            count = red[c, z, :, part : part + 1]
        prior = prior_ref[:, c * part : (c + 1) * part].astype(jnp.float32)
        fresh = jnp.where(count > 0.5, red[c, z, :, :part] / jnp.maximum(count, 1.0), prior)
        top = jnp.max(jnp.abs(fresh), axis=1, keepdims=True)
        power = jnp.ceil(jnp.log2(jnp.maximum(top, TINY)))
        code = jnp.floor(fresh * jnp.exp2(-power) * STEPS + 0.5).astype(jnp.int32)
        out_ref[c, own, :block] = (code[:, :code_w] << 16) | (code[:, code_w:] & 0xFFFF)
        at_row = lax.broadcasted_iota(jnp.int32, (block, LANES), 0)
        at_lane = lax.broadcasted_iota(jnp.int32, (block, LANES), 1)
        flat = jnp.sum(jnp.where(at_row == at_lane, power, 0.0), axis=0, keepdims=True)
        out_ref[c, own, block:] = jnp.zeros((EXTRA, code_w), jnp.int32)
        out_ref[c, own, block:, :LANES] = jnp.broadcast_to(flat.astype(jnp.int32), (EXTRA, LANES))

        @pl.when(z < last)
        def _(c=c):
            gright(c, z).start()

        @pl.when(z > 0)
        def _(c=c):
            gleft(c, z).start()

        xcopy(c, z, q).start()
        ycopy(c, z, q).start()
        return count

    def relay(c, n, by_x):
        if by_x:
            xcopy(c, n, nx).wait_recv()
        else:
            ycopy(c, n, ny).wait_recv()
        dcopy(c, n, by_x).start()

    def settle(c, n, by_x):
        if by_x:
            ycopy(c, n, ny).wait_recv()
        else:
            xcopy(c, n, nx).wait_recv()
        dcopy(c, n, by_x).wait_recv()

    def each(k, c, action):
        if k == 0:
            action(c, z, c % 2 == 0)
            return

        @pl.when(z >= k)
        def _():
            action(c, z - k, k % 2 == 0)

        @pl.when(z + k <= last)
        def _():
            action(c, z + k, k % 2 == 1)

    def spread(c, k):
        @pl.when(z >= k)
        def _():
            gright(c, z - k).wait_recv()

            @pl.when(z < last)
            def _():
                gright(c, z - k).start()

            xcopy(c, z - k, q).start()
            ycopy(c, z - k, q).start()

        @pl.when(z + k <= last)
        def _():
            gleft(c, z + k).wait_recv()

            @pl.when(z > 0)
            def _():
                gleft(c, z + k).start()

            xcopy(c, z + k, q).start()
            ycopy(c, z + k, q).start()

        each(k - 1, c, relay)

    open_gather(0)
    close_gather(0)
    for c in range(CHUNKS):
        if c + 1 < CHUNKS:
            open_gather(c + 1)
        combine(c)
        if c + 1 < CHUNKS:
            close_gather(c + 1)
    count = None
    for c in range(CHUNKS):
        count = publish(c, count)
    for k in range(1, z_n):
        for c in range(CHUNKS):
            spread(c, k)
    for c in range(CHUNKS):
        each(last, c, relay)
    for k in range(z_n):
        for c in range(CHUNKS):
            each(k, c, settle)

    for copy in id_copies + [ccopy] + mcopies:
        copy.wait_send()
    for c in range(CHUNKS):
        for copy in gathers[c]:
            copy.wait_send()
        for t in range(z_n):

            if t > 0:
                direct(c, t).wait_send()

            @pl.when((z >= t) & (z < last))
            def _(c=c, t=t):
                gright(c, t).wait_send()

            @pl.when((z <= t) & (z > 0))
            def _(c=c, t=t):
                gleft(c, t).wait_send()

            xcopy(c, t, q).wait_send()
            ycopy(c, t, q).wait_send()
            dcopy(c, t, True).wait_send()


def shards(points, centroids, assign, keep_mask):
    rows, width = points.shape
    shard_rows = centroids.shape[0]
    z_n = lax.axis_size("z")
    dp_n = z_n * PLANE
    block = shard_rows // dp_n
    own = lax.axis_index("z") * PLANE + lax.axis_index("q")
    ids = jnp.where(keep_mask > 0, assign, -1)
    ids = jnp.broadcast_to(ids[None, :], (8, rows))
    prior = lax.dynamic_slice_in_dim(centroids, own * block, block, 0)
    vmem = pl.BlockSpec(memory_space=pltpu.VMEM)
    dma = pltpu.SemaphoreType.DMA
    part = width // CHUNKS
    wide = part + LANES
    per = dma((CHUNKS, z_n))
    back, low = pl.pallas_call(
        functools.partial(update_kernel, z_n, shard_rows),
        out_shape=(
            jax.ShapeDtypeStruct((CHUNKS, dp_n, block + EXTRA, part // 2), jnp.int32),
            jax.ShapeDtypeStruct((8, rows), jnp.float32),
        ),
        in_specs=[vmem] * 4,
        out_specs=(vmem, vmem),
        scratch_shapes=[
            pltpu.VMEM((shard_rows, width), centroids.dtype),
            pltpu.VMEM((CHUNKS, 3, rows, part), points.dtype),
            pltpu.VMEM((3, 8, rows), jnp.int32),
            pltpu.VMEM((CHUNKS, 2 * z_n, block, wide), jnp.float32),
            pltpu.VMEM((CHUNKS, z_n, block, wide), jnp.float32),
            pltpu.VMEM((CHUNKS, z_n, block, wide), jnp.float32),
            pltpu.VMEM((CHUNKS, z_n, block, wide), jnp.float32),
            dma, dma, dma((3,)), dma((3,)), dma((CHUNKS, 6)), dma((CHUNKS, 6)),
            dma((CHUNKS,)), dma((CHUNKS,)),
            per, per, per, per, per, per, per, per, per, per, per, per,
        ],
        compiler_params=pltpu.CompilerParams(
            collective_id=0, has_side_effects=True, vmem_limit_bytes=56 * 1024 * 1024
        ),
        cost_estimate=pl.CostEstimate(
            flops=0, bytes_accessed=200 * 1024 * 1024, transcendentals=0
        ),
    )(points, ids, prior, centroids)
    codes = back[:, :, :block]
    powers = back[:, :, block, :block].astype(jnp.float32)
    scale = (jnp.exp2(powers) / STEPS)[:, :, :, None]
    pieces = []
    for c in range(CHUNKS):
        pieces += [(codes[c] >> 16) * scale[c], ((codes[c] << 16) >> 16) * scale[c]]
    new_centroids = jnp.concatenate(pieces, axis=2).reshape(shard_rows, width)
    point_f = points.astype(jnp.float32)
    point_sq = jnp.sum(point_f * point_f, axis=1)
    return new_centroids, (point_sq + low[0]) / width


def solution(mesh):
    dp, mp = mesh.shape["dp"], mesh.shape["mp"]
    grid = Mesh(mesh.devices.reshape(dp // PLANE, PLANE, mp), ("z", "q", "mp"))
    rows = ("z", "q", "mp")
    in_specs = (P(rows, None), P("mp", None), P(rows), P(rows))
    out_specs = (P("mp", None), P(rows))
    return jax.shard_map(shards, mesh=grid, in_specs=in_specs, out_specs=out_specs, check_vma=False)
```
